512 devices in a mesh: dom: 64 (over x, y, core), grp: 8 (over z).
Axes of the slice: x: 4, y: 8, z: 8, core: 2. Of those that a mesh axis runs over, the one named last changes fastest.
Arguments:
- tangent_tiles: bfloat16 [65536, 128, 128], P(('grp', 'dom')), parts along dimension 0, may hold values from -0.5 to 0.5
- tile_blocks: int32 [8192, 2], P('dom'), may hold values from 0 to 511, as said below
- block_home: int32 [512], replicated, may hold values from 0 to 511, as said below
- tile_count: int32 [64], P('dom'), may hold values from 48 to 128, as said below
- basis: bfloat16 [65536, 256], P('dom'), may hold values from -0.29882812 to 0.29882812
Outputs:
- reduced: float32 [2048, 256], P('grp'), parts along dimension 0
The draws below stay inside these ranges and needn't reach their ends.
There are 8 independent parts, one for each index of `grp`. The reference program is written for one: setup_inputs(seed, part) draws one part's arguments, and reference() takes and returns one part's arrays. A program takes and returns all parts, laid end to end along the dimension named above; an argument that names none is the same for every part. Nothing has to cross between parts.
Inputs may be any that keep to these rules, and one draw needn't show every extreme that they name: `tile_blocks`: every row block named by a device's tile slots has its position held by one of the devices with dom index from that device's index - 4 to its index + 8 // 2 - 1, taken cyclically. Among the row blocks named by one device's 128 slots, at most 2 distinct ones have their position held by any one device; every device reaches 2 for some holder. `block_home`: A permutation of the row blocks. `tile_count`: some device has exactly 128 live slots.
All inputs are finite; a program needn't handle non-finite values.
Results may differ from the reference program's by a relative error of at most 0.0029.
Values may be sent and summed in bfloat16 or wider, within the bound.
A program may use at most 64 MiB of HBM per device.

```python
import jax
import jax.numpy as jnp
from jax import lax

BLOCK = 128
RANK = 256
TILE_DEV = 128
BLK_DEV = 8
CAP = 2
NEAR = 8
NB = 512
TILES = 8192
N_DOM = 64


def layout_tables(key):
    home = jax.random.permutation(jax.random.fold_in(key, 11), NB).astype(jnp.int32)
    at_place = jnp.argsort(home, stable=True).astype(jnp.int32)
    device_ids = jnp.arange(N_DOM, dtype=jnp.int32)[:, None, None]
    steps_away = jax.random.randint(jax.random.fold_in(key, 12), (N_DOM, TILE_DEV, 2), 0, NEAR) - NEAR // 2
    owners = (device_ids + steps_away) % N_DOM
    shifts = jax.random.randint(jax.random.fold_in(key, 13), (N_DOM, N_DOM), 0, BLK_DEV)
    picks = jax.random.randint(jax.random.fold_in(key, 14), (N_DOM, TILE_DEV, 2), 0, CAP)
    owners = owners.at[:, 0, 1].set(owners[:, 0, 0])
    picks = picks.at[:, 0, 0].set(0)
    picks = picks.at[:, 0, 1].set(1)
    offset = shifts[device_ids, owners]
    place = owners * BLK_DEV + (offset + picks) % BLK_DEV
    linked = at_place[place].reshape(TILE_DEV * N_DOM, 2).astype(jnp.int32)
    return (home, linked)


def draw_tile_blocks(key, part):
    return layout_tables(key)[1]


def draw_block_home(key, part):
    return layout_tables(key)[0]


def draw_tile_count(key, part):
    counts = jax.random.randint(jax.random.fold_in(key, 21), (N_DOM,), 3 * TILE_DEV // 8, TILE_DEV + 1)
    busiest = jax.random.randint(jax.random.fold_in(key, 22), (), 0, N_DOM)
    counts = jnp.where(jnp.arange(N_DOM) == busiest, TILE_DEV, counts)
    return counts.astype(jnp.int32)


def levels(stream_key, extent, cuts, least, largest):
    gain, own = 1.0, jax.random.fold_in(stream_key, 6)
    for position, parts in cuts:
        steps = jnp.exp(jax.random.uniform(jax.random.fold_in(own, position), (parts,), jnp.float32, least / len(cuts), largest / len(cuts)))
        gain = gain * jnp.repeat(steps, extent[position] // parts).reshape([-1 if axis == position else 1 for axis in range(len(extent))])
    return gain


def gaussian(own_key, dims, width, limit, shards=(), kind=jnp.bfloat16):
    entries = jax.random.normal(own_key, dims, jnp.float32) * width
    if len(shards) > 0:
        entries = levels(own_key, dims, shards, -0.22, 0.18) * entries
    return jnp.clip(entries, min=-limit, max=limit).astype(kind)


def setup_inputs(seed: int = 0, part: int = 0) -> dict:
    arg_keys = jax.random.split(jax.random.key(seed), 6)
    own_keys = jax.random.split(jax.random.fold_in(arg_keys[5], part), 6)
    tangent_tiles = gaussian(own_keys[0], (TILES, BLOCK, BLOCK), BLOCK ** -0.5, 0.5, ((0, 64),))
    tile_blocks = draw_tile_blocks(jax.random.fold_in(arg_keys[5], 71), part)
    block_home = draw_block_home(jax.random.fold_in(arg_keys[5], 71), part)
    tile_count = draw_tile_count(jax.random.fold_in(arg_keys[5], 71), part)
    basis = gaussian(arg_keys[4], (NB * BLOCK, RANK), 0.05, 0.29882812, ((0, 64),))
    return {"tangent_tiles": tangent_tiles, "tile_blocks": tile_blocks, "block_home": block_home, "tile_count": tile_count, "basis": basis}


def reference(tangent_tiles, tile_blocks, block_home, tile_count, basis):
    stored = basis.reshape(NB, BLOCK, RANK)
    blocks = jnp.take(stored, block_home, axis=0)
    tiles = tangent_tiles.reshape(N_DOM, TILE_DEV, BLOCK, BLOCK)
    links = tile_blocks.reshape(N_DOM, TILE_DEV, 2)
    slots = jnp.arange(TILE_DEV, dtype=jnp.int32)

    def one_device(carry, items):
        tile_set, link_set, count = items
        live = (slots < count).astype(jnp.float32)
        cols = jnp.take(blocks, link_set[:, 1], axis=0).astype(jnp.float32)
        rows = jnp.take(blocks, link_set[:, 0], axis=0)
        right = jnp.einsum("tab,tbr->tar", tile_set.astype(jnp.float32), cols)
        right = (right * live[:, None, None]).astype(jnp.bfloat16)
        part = jnp.dot(rows.reshape(TILE_DEV * BLOCK, RANK).T, right.reshape(TILE_DEV * BLOCK, RANK), preferred_element_type=jnp.float32)
        return carry + part, None

    total, _ = lax.scan(one_device, jnp.zeros((RANK, RANK), jnp.float32), (tiles, links, tile_count))
    return total
```

```python
import functools

import jax
import jax.numpy as jnp
from jax import lax
from jax.experimental import pallas as pl
from jax.experimental.pallas import tpu as pltpu
from jax.sharding import PartitionSpec as P

NEAR = 8
HALF = NEAR // 2
ORDER = (2, 6, 3, 5, 1, 7, 0)
UNROLL = 8


def remote(src, dst, send, recv, where):
    return pltpu.make_async_remote_copy(
        src_ref=src,
        dst_ref=dst,
        send_sem=send,
        recv_sem=recv,
        device_id={"dom": where},
        device_id_type=pl.DeviceIdType.MESH,
    )


def kernel(
    ndom,
    links_ref,
    home_ref,
    count_ref,
    tiles_hbm,
    basis_hbm,
    out_ref,
    tiles,
    stored,
    req_out,
    req_in,
    serve,
    fetched,
    turned,
    slots_v,
    slots,
    total,
    parts,
    came,
    final,
    tile_sem,
    basis_sem,
    slot_sem,
    req_send,
    req_recv,
    blk_send,
    blk_recv,
    sum_send,
    sum_recv,
    all_send,
    all_recv,
):
    me = lax.axis_index("dom")
    mask = ndom - 1

    basis_copy = pltpu.make_async_copy(basis_hbm, stored, basis_sem)
    basis_copy.start()
    tile_copy = pltpu.make_async_copy(tiles_hbm, tiles, tile_sem)
    tile_copy.start()

    barrier = pltpu.get_barrier_semaphore()

    def greet(k, carry):
        other = (me + k) & mask
        pl.semaphore_signal(barrier, inc=1, device_id={"dom": other}, device_id_type=pl.DeviceIdType.MESH)
        return carry

    lax.fori_loop(1, ndom, greet, 0)

    sub = lax.broadcasted_iota(jnp.int32, (8, 128), 0)

    def looked_up(row):
        ids = jnp.broadcast_to(links_ref[row : row + 1, :], (8, 128))
        place = jnp.zeros((8, 128), jnp.int32)
        for k in range(home_ref.shape[0]):
            table = jnp.broadcast_to(home_ref[k : k + 1, :], (8, 128))
            got = jnp.take_along_axis(table, ids & 127, axis=1)
            place = jnp.where((ids >> 7) == k, got, place)
        window = ((place >> 3) - me + HALF + ndom) & mask
        return window, place & 7, window == sub

    row_win, row_id, row_hit = looked_up(0)
    col_win, col_id, col_hit = looked_up(1)
    low = jnp.minimum(jnp.where(row_hit, row_id, 7), jnp.where(col_hit, col_id, 7))
    high = jnp.maximum(jnp.where(row_hit, row_id, 0), jnp.where(col_hit, col_id, 0))
    low = jnp.broadcast_to(jnp.min(low, axis=1, keepdims=True), (8, 128))
    high = jnp.broadcast_to(jnp.max(high, axis=1, keepdims=True), (8, 128))
    packed = low + 16 * high
    for w in range(NEAR):
        req_out[w] = jnp.broadcast_to(packed[w : w + 1, :], (8, 128))

    def slot_of(window, ids, hit):
        level = jnp.sum(jnp.where(hit & (ids != low), 1, 0), axis=0, keepdims=True)
        return jnp.minimum(2 * window[0:1] + level, 2 * NEAR - 1)

    row_slot = slot_of(row_win, row_id, row_hit)
    col_slot = slot_of(col_win, col_id, col_hit)
    lane = lax.broadcasted_iota(jnp.int32, (1, 128), 1)
    col_slot = jnp.where(lane < count_ref[0], col_slot, 2 * NEAR)
    slots_v[0:1, :] = row_slot
    slots_v[1:2, :] = col_slot
    slot_copy = pltpu.make_async_copy(slots_v, slots, slot_sem)
    slot_copy.start()

    pl.semaphore_wait(barrier, ndom - 1)

    def holder_of(w):
        return (me + (w - HALF + ndom)) & mask

    def asker_of(w):
        return (me + (HALF - w + ndom)) & mask

    for w in ORDER:
        remote(req_out.at[w], req_in.at[w], req_send.at[w], req_recv.at[w], holder_of(w)).start()

    basis_copy.wait()
    own = packed[HALF, 0]
    fetched[2 * HALF] = stored[own & 7]
    fetched[2 * HALF + 1] = stored[(own >> 4) & 7]
    fetched[2 * NEAR] = jnp.zeros(fetched.shape[1:], fetched.dtype)

    for w in ORDER:
        remote(req_out.at[w], req_in.at[w], req_send.at[w], req_recv.at[w], asker_of(w)).wait_recv()
        asked = req_in[w, 0, 0]
        serve[w, 0] = stored[asked & 7]
        serve[w, 1] = stored[(asked >> 4) & 7]
        remote(serve.at[w], fetched.at[pl.ds(2 * w, 2)], blk_send.at[w], blk_recv.at[w], asker_of(w)).start()

    for w in (HALF,) + ORDER:
        if w != HALF:
            remote(serve.at[w], fetched.at[pl.ds(2 * w, 2)], blk_send.at[w], blk_recv.at[w], holder_of(w)).wait_recv()
        turned[2 * w] = fetched[2 * w].T
        turned[2 * w + 1] = fetched[2 * w + 1].T

    slot_copy.wait()
    tile_copy.wait()
    total[...] = jnp.zeros_like(total)

    def project(step, carry):
        lefts, rights = [], []
        for u in range(UNROLL):
            t = step * UNROLL + u
            right = jnp.dot(tiles[t], fetched[slots[1, t]], preferred_element_type=jnp.float32)
            rights.append(right.astype(jnp.bfloat16))
            lefts.append(turned[slots[0, t]])
        total[...] += jnp.dot(
            jnp.concatenate(lefts, axis=1), jnp.concatenate(rights, axis=0), preferred_element_type=jnp.float32
        )
        return carry

    lax.fori_loop(0, tiles.shape[0] // UNROLL, project, 0)

    def cut(g, carry):
        rows = total[pl.ds(pl.multiple_of(g * 8, 8), 8), :].astype(jnp.bfloat16)
        parts[2 * g] = rows[:, :128]
        parts[2 * g + 1] = rows[:, 128:]
        return carry

    lax.fori_loop(0, ndom // 2, cut, 0)

    def send_part(k, carry):
        other = (me + k) & mask
        remote(parts.at[other], came.at[me], sum_send, sum_recv, other).start()
        return carry

    lax.fori_loop(1, ndom, send_part, 0)
    came[me] = parts[me]
    others = pl.ds(0, ndom - 1)
    remote(came.at[others], came.at[others], sum_send, sum_recv, me).wait_recv()
    summed = jnp.sum(came[...].astype(jnp.float32), axis=0)
    final[me] = summed.astype(jnp.bfloat16)

    def send_sum(k, carry):
        other = (me + k) & mask
        remote(final.at[me], final.at[me], all_send, all_recv, other).start()
        return carry

    lax.fori_loop(1, ndom, send_sum, 0)
    remote(final.at[others], final.at[others], all_send, all_recv, me).wait_recv()

    def put(g, carry):
        at = pl.ds(pl.multiple_of(g * 8, 8), 8)
        out_ref[at, 0:128] = final[2 * g].astype(jnp.float32)
        out_ref[at, 128:256] = final[2 * g + 1].astype(jnp.float32)
        return carry

    lax.fori_loop(0, ndom // 2, put, 0)

    for w in ORDER:
        remote(req_out.at[w], req_in.at[w], req_send.at[w], req_recv.at[w], holder_of(w)).wait_send()
        remote(serve.at[w], fetched.at[pl.ds(2 * w, 2)], blk_send.at[w], blk_recv.at[w], asker_of(w)).wait_send()
    remote(parts.at[others], parts.at[others], sum_send, sum_recv, me).wait_send()
    remote(final.at[others], final.at[others], all_send, all_recv, me).wait_send()


def solution(mesh):
    ndom = mesh.shape["dom"]

    def on_device(tangent_tiles, tile_blocks, block_home, tile_count, basis):
        count, block = tangent_tiles.shape[:2]
        rank = basis.shape[1]
        held = basis.shape[0] // block
        bf16, f32, i32 = jnp.bfloat16, jnp.float32, jnp.int32
        vmem, dma = pltpu.VMEM, pltpu.SemaphoreType.DMA
        return pl.pallas_call(
            functools.partial(kernel, ndom),
            out_shape=jax.ShapeDtypeStruct((rank, rank), f32),
            in_specs=[
                pl.BlockSpec(memory_space=pltpu.VMEM),
                pl.BlockSpec(memory_space=pltpu.VMEM),
                pl.BlockSpec(memory_space=pltpu.SMEM),
                pl.BlockSpec(memory_space=pl.ANY),
                pl.BlockSpec(memory_space=pl.ANY),
            ],
            out_specs=pl.BlockSpec(memory_space=pltpu.VMEM),
            scratch_shapes=[
                vmem((count, block, block), bf16),
                vmem((held, block, rank), bf16),
                vmem((NEAR, 8, 128), i32),
                vmem((NEAR, 8, 128), i32),
                vmem((NEAR, 2, block, rank), bf16),
                vmem((2 * NEAR + 1, block, rank), bf16),
                vmem((2 * NEAR, rank, block), bf16),
                vmem((2, 128), i32),
                pltpu.SMEM((2, 128), i32),
                vmem((rank, rank), f32),
                vmem((ndom, 8, 128), bf16),
                vmem((ndom, 8, 128), bf16),
                vmem((ndom, 8, 128), bf16),
                dma,
                dma,
                dma,
                dma((NEAR,)),
                dma((NEAR,)),
                dma((NEAR,)),
                dma((NEAR,)),
                dma,
                dma,
                dma,
                dma,
            ],
            compiler_params=pltpu.CompilerParams(
                collective_id=0, has_side_effects=True
            ),
        )(
            tile_blocks.T,
            block_home.reshape(-1, 128),
            tile_count,
            tangent_tiles,
            basis.reshape(held, block, rank),
        )

    return jax.shard_map(
        on_device,
        mesh=mesh,
        in_specs=(P(("grp", "dom"), None, None), P("dom", None), P(), P("dom"), P("dom", None)),
        out_specs=P("grp", None),
        check_vma=False,
    )
```

```python
import functools

import jax
import jax.numpy as jnp
from jax import lax
from jax.experimental import pallas as pl
from jax.experimental.pallas import tpu as pltpu
from jax.sharding import PartitionSpec as P

NEAR = 8
HALF = NEAR // 2
DIRECT = (2, 6, 3, 5)
UNROLL = 8
TEAM = 4
GRP = 8


def remote(src, dst, send, recv, where):
    return pltpu.make_async_remote_copy(
        src_ref=src,
        dst_ref=dst,
        send_sem=send,
        recv_sem=recv,
        device_id=where,
        device_id_type=pl.DeviceIdType.MESH,
    )


def signal(sem, where):
    pl.semaphore_signal(sem, inc=1, device_id=where, device_id_type=pl.DeviceIdType.MESH)


def team_of(depth, team):
    place = (depth + 2 * team) & (TEAM - 1)
    first = depth - place + GRP
    others = [(first + ((place + k) & (TEAM - 1))) & (GRP - 1) for k in range(1, TEAM)]
    return place, others


def kernel(
    ndom,
    links_ref,
    home_ref,
    count_ref,
    tiles_hbm,
    basis_hbm,
    out_ref,
    tiles,
    stored,
    req_out,
    req_in,
    serve,
    serve_part,
    fetched,
    turned,
    slots_v,
    slots,
    total,
    parts,
    came,
    final,
    tile_sem,
    basis_sem,
    slot_sem,
    req_send,
    req_recv,
    blk_send,
    blk_recv,
    far_send,
    far_recv,
    pass_send,
    pass_recv,
    round_sem,
    sum_send,
    sum_recv,
    all_send,
    all_recv,
):
    me = lax.axis_index("dom")
    depth = lax.axis_index("grp")
    mask = ndom - 1
    core = me & 1

    basis_copy = pltpu.make_async_copy(basis_hbm, stored, basis_sem)
    basis_copy.start()
    tile_copy = pltpu.make_async_copy(tiles_hbm, tiles, tile_sem)
    tile_copy.start()

    barrier = pltpu.get_barrier_semaphore()
    for step in range(1, HALF + 1):
        for other in ((me + step) & mask, (me - step + ndom) & mask):
            signal(barrier, {"dom": other})
    for team in (0, 1):
        for other in team_of(depth, team)[1]:
            signal(barrier, {"grp": other})

    sub = lax.broadcasted_iota(jnp.int32, (8, 128), 0)

    def looked_up(row):
        ids = jnp.broadcast_to(links_ref[row : row + 1, :], (8, 128))
        place = jnp.zeros((8, 128), jnp.int32)
        for k in range(home_ref.shape[0]):
            table = jnp.broadcast_to(home_ref[k : k + 1, :], (8, 128))
            got = jnp.take_along_axis(table, ids & 127, axis=1)
            place = jnp.where((ids >> 7) == k, got, place)
        window = ((place >> 3) - me + HALF + ndom) & mask
        return window, place & 7, window == sub

    row_win, row_id, row_hit = looked_up(0)
    col_win, col_id, col_hit = looked_up(1)
    low = jnp.minimum(jnp.where(row_hit, row_id, 7), jnp.where(col_hit, col_id, 7))
    high = jnp.maximum(jnp.where(row_hit, row_id, 0), jnp.where(col_hit, col_id, 0))
    low = jnp.broadcast_to(jnp.min(low, axis=1, keepdims=True), (8, 128))
    high = jnp.broadcast_to(jnp.max(high, axis=1, keepdims=True), (8, 128))
    packed = low + 16 * high
    for w in range(NEAR):
        req_out[w] = jnp.broadcast_to(packed[w : w + 1, :], (8, 128))

    def slot_of(window, ids, hit):
        level = jnp.sum(jnp.where(hit & (ids != low), 1, 0), axis=0, keepdims=True)
        return jnp.minimum(2 * window[0:1] + level, 2 * NEAR - 1)

    row_slot = slot_of(row_win, row_id, row_hit)
    col_slot = slot_of(col_win, col_id, col_hit)
    lane = lax.broadcasted_iota(jnp.int32, (1, 128), 1)
    col_slot = jnp.where(lane < count_ref[0], col_slot, 2 * NEAR)
    slots_v[0:1, :] = row_slot
    slots_v[1:2, :] = col_slot
    slot_copy = pltpu.make_async_copy(slots_v, slots, slot_sem)
    slot_copy.start()

    pl.semaphore_wait(barrier, 2 * HALF + 2 * (TEAM - 1))

    def holder_of(w):
        return (me + (w - HALF + ndom)) & mask

    def asker_of(w):
        return (me + (HALF - w + ndom)) & mask

    rows_far = fetched.shape[1] // TEAM
    ask_far = (0, 1 + 6 * core)
    ask_near = DIRECT + (7 - 6 * core,)
    serve_far = (0, 7 - 6 * core)
    serve_near = DIRECT + (1 + 6 * core,)

    def share(ref, w, team, place):
        at = pl.ds(pl.multiple_of(place * rows_far, rows_far), rows_far)
        return ref.at[pl.ds(2 * w, 2), at]

    def request(w, where):
        return remote(req_out.at[w], req_in.at[w], req_send.at[w], req_recv.at[w], {"dom": where})

    def far(n, w, where):
        place = team_of(depth, n)[0]
        part = share(fetched, w, n, place)
        return remote(serve_part.at[n], part, far_send.at[n], far_recv.at[n], {"dom": where})

    def near(n, w, where):
        return remote(serve.at[n], fetched.at[pl.ds(2 * w, 2)], blk_send.at[n], blk_recv.at[n], {"dom": where})

    def pass_on(n, w, k):
        place, others = team_of(depth, n)
        part = share(fetched, w, n, place)
        return remote(part, part, pass_send.at[n, k], pass_recv.at[n], {"grp": others[k]})

    for w in ask_far + ask_near:
        request(w, holder_of(w)).start()
    for other in ((me + HALF) & mask, (me - HALF + ndom) & mask):
        signal(round_sem.at[0], {"dom": other})

    basis_copy.wait()
    own = packed[HALF, 0]
    fetched[2 * HALF] = stored[own & 7]
    fetched[2 * HALF + 1] = stored[(own >> 4) & 7]
    fetched[2 * NEAR] = jnp.zeros(fetched.shape[1:], fetched.dtype)

    for n, w in enumerate(serve_far):
        request(w, asker_of(w)).wait_recv()
        asked = req_in[w, 0, 0]
        at = pl.ds(pl.multiple_of(team_of(depth, n)[0] * rows_far, rows_far), rows_far)
        serve_part[n, 0] = stored[asked & 7, at]
        serve_part[n, 1] = stored[(asked >> 4) & 7, at]
        far(n, w, asker_of(w)).start()
    for n, w in enumerate(serve_near):
        request(w, asker_of(w)).wait_recv()
        asked = req_in[w, 0, 0]
        serve[n, 0] = stored[asked & 7]
        serve[n, 1] = stored[(asked >> 4) & 7]
        near(n, w, asker_of(w)).start()

    def meet(n, gap):
        pl.semaphore_wait(round_sem.at[n], 2)
        for other in ((me + gap) & mask, (me - gap + ndom) & mask):
            signal(round_sem.at[n + 1], {"dom": other})

    meet(0, 2 * HALF)
    for n, w in enumerate(ask_far):
        far(n, w, holder_of(w)).wait_recv()
        for k in range(TEAM - 1):
            pass_on(n, w, k).start()
    meet(1, 4 * HALF)

    def turn(w):
        turned[2 * w] = fetched[2 * w].T
        turned[2 * w + 1] = fetched[2 * w + 1].T

    turn(HALF)
    for n, w in enumerate(ask_near):
        near(n, w, holder_of(w)).wait_recv()
        turn(w)
    for n, w in enumerate(ask_far):
        rest = fetched.at[pl.ds(2 * w, 2), pl.ds(0, (TEAM - 1) * rows_far)]
        remote(rest, rest, pass_send.at[n, 0], pass_recv.at[n], {"dom": me}).wait_recv()
        turn(w)
    pl.semaphore_wait(round_sem.at[2], 2)

    slot_copy.wait()
    tile_copy.wait()
    total[...] = jnp.zeros_like(total)

    def project(step, carry):
        lefts, rights = [], []
        for u in range(UNROLL):
            t = step * UNROLL + u
            right = jnp.dot(tiles[t], fetched[slots[1, t]], preferred_element_type=jnp.float32)
            rights.append(right.astype(jnp.bfloat16))
            lefts.append(turned[slots[0, t]])
        total[...] += jnp.dot(
            jnp.concatenate(lefts, axis=1), jnp.concatenate(rights, axis=0), preferred_element_type=jnp.float32
        )
        return carry

    lax.fori_loop(0, tiles.shape[0] // UNROLL, project, 0)

    def cut(g, carry):
        rows = total[pl.ds(pl.multiple_of(g * 8, 8), 8), :].astype(jnp.bfloat16)
        parts[2 * g] = rows[:, :128]
        parts[2 * g + 1] = rows[:, 128:]
        return carry

    lax.fori_loop(0, ndom // 2, cut, 0)

    def apart(k):
        return ndom // 2 + (k >> 1) * (1 - 2 * (k & 1))

    def send_part(k, carry):
        other = (me + apart(k)) & mask
        remote(parts.at[other], came.at[me], sum_send, sum_recv, {"dom": other}).start()
        return carry

    lax.fori_loop(1, ndom, send_part, 0)
    came[me] = parts[me]
    others = pl.ds(0, ndom - 1)
    remote(came.at[others], came.at[others], sum_send, sum_recv, {"dom": me}).wait_recv()
    summed = jnp.sum(came[...].astype(jnp.float32), axis=0)
    final[me] = summed.astype(jnp.bfloat16)

    def send_sum(k, carry):
        other = (me + apart(k)) & mask
        remote(final.at[me], final.at[me], all_send, all_recv, {"dom": other}).start()
        return carry

    lax.fori_loop(1, ndom, send_sum, 0)
    remote(final.at[others], final.at[others], all_send, all_recv, {"dom": me}).wait_recv()

    def put(g, carry):
        at = pl.ds(pl.multiple_of(g * 8, 8), 8)
        out_ref[at, 0:128] = final[2 * g].astype(jnp.float32)
        out_ref[at, 128:256] = final[2 * g + 1].astype(jnp.float32)
        return carry

    lax.fori_loop(0, ndom // 2, put, 0)

    for w in ask_far + ask_near:
        request(w, holder_of(w)).wait_send()
    for n, w in enumerate(serve_near):
        near(n, w, asker_of(w)).wait_send()
    for n, w in enumerate(serve_far):
        far(n, w, asker_of(w)).wait_send()
    for n, w in enumerate(ask_far):
        for k in range(TEAM - 1):
            pass_on(n, w, k).wait_send()
    remote(parts.at[others], parts.at[others], sum_send, sum_recv, {"dom": me}).wait_send()
    remote(final.at[others], final.at[others], all_send, all_recv, {"dom": me}).wait_send()


def solution(mesh):
    ndom = mesh.shape["dom"]

    def on_device(tangent_tiles, tile_blocks, block_home, tile_count, basis):
        count, block = tangent_tiles.shape[:2]
        rank = basis.shape[1]
        held = basis.shape[0] // block
        bf16, f32, i32 = jnp.bfloat16, jnp.float32, jnp.int32
        vmem, dma = pltpu.VMEM, pltpu.SemaphoreType.DMA
        return pl.pallas_call(
            functools.partial(kernel, ndom),
            out_shape=jax.ShapeDtypeStruct((rank, rank), f32),
            in_specs=[
                pl.BlockSpec(memory_space=pltpu.VMEM),
                pl.BlockSpec(memory_space=pltpu.VMEM),
                pl.BlockSpec(memory_space=pltpu.SMEM),
                pl.BlockSpec(memory_space=pl.ANY),
                pl.BlockSpec(memory_space=pl.ANY),
            ],
            out_specs=pl.BlockSpec(memory_space=pltpu.VMEM),
            scratch_shapes=[
                vmem((count, block, block), bf16),
                vmem((held, block, rank), bf16),
                vmem((NEAR, 8, 128), i32),
                vmem((NEAR, 8, 128), i32),
                vmem((len(DIRECT) + 1, 2, block, rank), bf16),
                vmem((2, 2, block // TEAM, rank), bf16),
                vmem((2 * NEAR + 1, block, rank), bf16),
                vmem((2 * NEAR, rank, block), bf16),
                vmem((2, 128), i32),
                pltpu.SMEM((2, 128), i32),
                vmem((rank, rank), f32),
                vmem((ndom, 8, 128), bf16),
                vmem((ndom, 8, 128), bf16),
                vmem((ndom, 8, 128), bf16),
                dma,
                dma,
                dma,
                dma((NEAR,)),
                dma((NEAR,)),
                dma((len(DIRECT) + 1,)),
                dma((len(DIRECT) + 1,)),
                dma((2,)),
                dma((2,)),
                dma((2, TEAM - 1)),
                dma((2,)),
                pltpu.SemaphoreType.REGULAR((3,)),
                dma,
                dma,
                dma,
                dma,
            ],
            compiler_params=pltpu.CompilerParams(
                collective_id=0, has_side_effects=True
            ),
        )(
            tile_blocks.T,
            block_home.reshape(-1, 128),
            tile_count,
            tangent_tiles,
            basis.reshape(held, block, rank),
        )

    return jax.shard_map(
        on_device,
        mesh=mesh,
        in_specs=(P(("grp", "dom"), None, None), P("dom", None), P(), P("dom"), P("dom", None)),
        out_specs=P("grp", None),
        check_vma=False,
    )
```
